32 devices in a mesh: expert: 8 (over z, y), helper: 4 (over x, core).
Axes of the slice: x: 2, y: 2, z: 4, core: 2. Of those that a mesh axis runs over, the one named last changes fastest.
Arguments:
- tokens: bfloat16 [32768, 768], P(('expert', 'helper')), may hold values from -6 to 6
- gate: float32 [32768], P(('expert', 'helper')), may hold values from 0.2 to 1
- expert_ids: int32 [32768, 1], P(('expert', 'helper')), may hold values from 0 to 31; in each aligned block of 1024 rows (0 to 1023, 1024 to 2047, ...) at most 48 rows name the same one
- backup_ids: int32 [32768, 1], P(('expert', 'helper')), may hold values from 0 to 31; in each aligned block of 1024 rows (0 to 1023, 1024 to 2047, ...) at most 48 rows name the same one
- capacity: int32 [32], replicated, may hold values from 2 to 48
- w_in: bfloat16 [32, 768, 3072], P('expert', None, 'helper'), may hold values from -0.21875 to 0.21875
- w_out: bfloat16 [32, 3072, 768], P('expert', 'helper'), may hold values from -0.109375 to 0.109375
Outputs:
- mixed: bfloat16 [32768, 768], P(('expert', 'helper'))
The draws below stay inside these ranges and needn't reach their ends.
Inputs may be any that keep to these rules, and one draw needn't show every extreme that they name: `expert_ids`: in the rows of one device no expert is the first expert of more than 48 rows; some expert reaches 48. `backup_ids`: in the rows of one device no expert is the backup of more than 48 rows; some expert reaches 48.
All inputs are finite; a program needn't handle non-finite values.
Results may differ from the reference program's by a relative error of at most 0.0095.
Values may be sent and summed in bfloat16 or wider, within the bound.
A program may use at most 192 MiB of HBM per device.

```python
import math
import jax
import jax.numpy as jnp
import numpy as np
from jax import lax

D = 768
FF = 3072
TOK_DEV = 1024
EXPERTS = 32
SLOT = 48
TOKENS = 32768
N_EXPERT = 8
N_HELPER = 4


def touch_ends(entries, stream_key, low, largest):
    place = [jax.random.randint(jax.random.fold_in(stream_key, axis), (), 0, length) for axis, length in enumerate(entries.shape)]
    longest = entries.shape.index(max(entries.shape))
    next_to = place[:longest] + [(place[longest] + 1) % entries.shape[longest]] + place[longest + 1:]
    return entries.at[tuple(place)].set(low).at[tuple(next_to)].set(largest)


def level_of(own_key, extent, pieces, smallest, high):
    def one(axis_at, blocks):
        steps = jax.random.uniform(jax.random.fold_in(jax.random.fold_in(own_key, 6), axis_at), (blocks,), jnp.float32, smallest / len(pieces), high / len(pieces))
        return jnp.repeat(jnp.exp(steps), extent[axis_at] // blocks).reshape((-1,) + (1,) * (len(extent) - axis_at - 1))

    loudness = one(*pieces[0])
    for cut in pieces[1:]:
        loudness = loudness * one(*cut)
    return loudness


def shared_out(stream_key, own, number, rows, count, top, reach, skew):
    sequence = jax.random.permutation(stream_key, count)
    crowded, ordinary = shares(count, rows * top, reach, skew, True), shares(count, rows * top, reach, skew, False)
    places = jnp.arange(count)

    def named(tallies, turn):
        used = int((tallies > 0).sum())
        fixed = max(1, used // 4)
        shifted = fixed + (places - fixed + turn * (used - fixed)) % max(1, count - fixed)
        return jnp.zeros((count,), jnp.int32).at[sequence[jnp.where(places < fixed, places, shifted)]].set(jnp.asarray(tallies, jnp.int32))

    tallies = jnp.where(number % 4 == 0, named(crowded, number // 4), named(ordinary, number - number // 4 - 1))
    mixed = jax.random.permutation(jax.random.fold_in(own, 3), count)
    giver, receiver = mixed[0:count // 2 * 2:2], mixed[1:count // 2 * 2:2]
    margin = jnp.minimum(tallies[giver] - 1, reach - tallies[receiver]) // 2
    margin = jnp.where((giver == sequence[0]) | (receiver == sequence[0]) | (tallies[receiver] == 0), 0, jnp.maximum(margin, 0))
    shifted = jax.random.randint(jax.random.fold_in(own, 4), (count // 2,), 0, 1 << 20) % (margin + 1)
    tallies = tallies.at[giver].add(-shifted).at[receiver].add(shifted)
    items = jnp.searchsorted(jnp.cumsum(tallies), jnp.arange(rows * top), side="right").astype(jnp.int32)
    listing = items.reshape(top, rows).T
    listing = listing[jax.random.permutation(jax.random.fold_in(own, 1), rows)]
    turn = jax.random.randint(jax.random.fold_in(own, 2), (rows, 1), 0, top)
    return jnp.take_along_axis(listing, (jnp.arange(top)[None, :] + turn) % top, axis=1)


def shares(amount, total, reach, lean, full):
    portions = [(1 << 20) // math.isqrt(rank ** lean) + 1 for rank in range(1, amount + 1)]
    largest = reach if full else min(reach, max(-(-total // amount), total * portions[0] // sum(portions)))
    least = 1 if total - largest >= amount - 1 else 0
    counts, surplus = [largest] + [least] * (amount - 1), total - largest - least * (amount - 1)
    while surplus > 0:
        free = [i for i in range(1, amount) if counts[i] < largest] or [i for i in range(1, amount) if counts[i] < reach]
        whole, budget = sum([portions[i] for i in free]), surplus
        for i in free:
            extra = min(reach - counts[i], max(1, budget * portions[i] // whole), surplus)
            counts[i] = counts[i] + extra
            surplus = surplus - extra
    return np.array(counts)


def centred(stream_key, shape, scale, most, pieces=(), kind=jnp.bfloat16):
    level = level_of(stream_key, shape, pieces, -0.22, 0.18) if pieces else 1.0
    values = jax.random.normal(stream_key, shape, jnp.float32) * scale * level
    return jnp.minimum(jnp.maximum(values, -most), most).astype(kind)


def setup_inputs(seed: int = 0) -> dict:
    arg_keys = jax.random.split(jax.random.key(seed), 8)
    tokens = centred(arg_keys[0], (TOKENS, D), 1.0, 6.0, ((0, 32),))
    gate = jnp.clip(0.2 + 0.8 * jax.random.uniform(arg_keys[1], (TOKENS,), jnp.float32) ** level_of(arg_keys[1], (TOKENS,), ((0, 32),), -0.2, 0.2), 0.2, 1.0)
    expert_ids_keys = jax.random.split(jax.random.fold_in(arg_keys[2], 1), TOKENS // TOK_DEV)
    expert_ids_turns = jax.random.permutation(jax.random.fold_in(arg_keys[2], 3), TOKENS // TOK_DEV)
    expert_ids = jax.vmap(lambda own, number: shared_out(jax.random.fold_in(arg_keys[2], 2), own, number, TOK_DEV, EXPERTS, 1, SLOT, 2))(expert_ids_keys, expert_ids_turns).reshape((TOKENS, 1))
    backup_ids_keys = jax.random.split(jax.random.fold_in(arg_keys[3], 1), TOKENS // TOK_DEV)
    backup_ids_turns = jax.random.permutation(jax.random.fold_in(arg_keys[3], 3), TOKENS // TOK_DEV)
    backup_ids = jax.vmap(lambda own, number: shared_out(jax.random.fold_in(arg_keys[3], 2), own, number, TOK_DEV, EXPERTS, 1, SLOT, 1))(backup_ids_keys, backup_ids_turns).reshape((TOKENS, 1))
    capacity = touch_ends(jax.random.randint(arg_keys[4], (EXPERTS,), 2, SLOT + 1), jax.random.fold_in(arg_keys[4], 1), 2, SLOT).astype(jnp.int32)
    w_in = centred(arg_keys[5], (EXPERTS, D, FF), D ** -0.5, 0.21875, ((0, 8), (2, 4)))
    w_out = centred(arg_keys[6], (EXPERTS, FF, D), FF ** -0.5, 0.109375, ((0, 8), (1, 4)))
    return dict(tokens=tokens, gate=gate, expert_ids=expert_ids, backup_ids=backup_ids, capacity=capacity, w_in=w_in, w_out=w_out)


def assign(first, backup, capacity, count, slot):
    columns = jnp.arange(count, dtype=jnp.int32)
    onehot = (first[:, None] == columns[None, :]).astype(jnp.int32)
    rank = jnp.sum((jnp.cumsum(onehot, axis=0) - onehot) * onehot, axis=1)
    limit = jnp.sum(onehot * capacity[None, :], axis=1)
    kept = rank < limit
    spill = (backup[:, None] == columns[None, :]).astype(jnp.int32) * (1 - kept.astype(jnp.int32))[:, None]
    spill_rank = jnp.sum((jnp.cumsum(spill, axis=0) - spill) * spill, axis=1)
    final = jnp.where(kept, first, backup).astype(jnp.int32)
    slots = jnp.where(kept, rank, slot + spill_rank).astype(jnp.int32)
    return slots, final


def expert_apply(rows, weight_in, weight_out):
    width = weight_in.shape[1] // N_HELPER
    total = jnp.zeros((rows.shape[0], rows.shape[1]), jnp.float32)
    for quarter in range(N_HELPER):
        inner = weight_in[:, quarter * width:(quarter + 1) * width].astype(jnp.float32)
        outer = weight_out[quarter * width:(quarter + 1) * width, :].astype(jnp.float32)
        hidden = jax.nn.relu(jnp.dot(rows.astype(jnp.float32), inner)).astype(jnp.bfloat16)
        part = jnp.dot(hidden.astype(jnp.float32), outer).astype(jnp.bfloat16)
        total = total + part.astype(jnp.float32)
    return total.astype(jnp.bfloat16)


def reference(tokens, gate, expert_ids, backup_ids, capacity, w_in, w_out):
    devices = N_EXPERT * N_HELPER
    room = 2 * SLOT
    first = expert_ids[:, 0].reshape(devices, TOK_DEV)
    backup = backup_ids[:, 0].reshape(devices, TOK_DEV)
    slots, final = jax.vmap(lambda a, b: assign(a, b, capacity, EXPERTS, SLOT))(first, backup)
    owner = jnp.arange(devices, dtype=jnp.int32)[:, None] * room + slots
    owner = owner.reshape(-1)
    final = final.reshape(-1)
    buffer = jnp.zeros((EXPERTS, devices * room, D), jnp.bfloat16).at[final, owner].set(tokens)
    results = lax.map(lambda item: expert_apply(item[0], item[1], item[2]), (buffer, w_in, w_out))
    picked = results[final, owner]
    return (gate[:, None] * picked.astype(jnp.float32)).astype(jnp.bfloat16)
```

```python
import jax
import jax.numpy as jnp
from jax import lax
from jax.sharding import PartitionSpec as P


def ranks(onehot):
    rows = onehot.shape[0]
    earlier = lax.broadcasted_iota(jnp.int32, (rows, rows), 0) > lax.broadcasted_iota(
        jnp.int32, (rows, rows), 1
    )
    counts = jnp.dot(
        earlier.astype(jnp.bfloat16),
        onehot.astype(jnp.bfloat16),
        preferred_element_type=jnp.float32,
    )
    return jnp.sum(jnp.where(onehot, counts, 0.0), axis=1).astype(jnp.int32)


def assign(first, backup, capacity, count, slot):
    columns = jnp.arange(count, dtype=jnp.int32)
    onehot = first[:, None] == columns[None, :]
    rank = ranks(onehot)
    limit = jnp.sum(jnp.where(onehot, capacity[None, :], 0), axis=1)
    kept = rank < limit
    spill = (backup[:, None] == columns[None, :]) & ~kept[:, None]
    spill_rank = ranks(spill)
    final = jnp.where(kept, first, backup)
    slots = jnp.where(kept, rank, slot + spill_rank)
    return slots, final


def on_device(tokens, gate, expert_ids, backup_ids, capacity, w_in, w_out):
    held = w_in.shape[0]
    owners = lax.axis_size("expert")
    experts = held * owners
    rows, width = tokens.shape
    slot = max(6, 3 * rows // (2 * experts))
    room = 2 * slot

    gathered = []
    for expert in range(held):
        gathered.append(
            (
                lax.all_gather(w_in[expert], "helper", axis=1, tiled=True),
                lax.all_gather(w_out[expert], "helper", axis=0, tiled=True),
            )
        )

    slots, final = assign(expert_ids[:, 0], backup_ids[:, 0], capacity, experts, slot)
    place = (final // held) * room + slots
    which = final % held

    arrived = []
    for expert in range(held):
        target = jnp.where(which == expert, place, -1)
        hot = lax.broadcasted_iota(jnp.int32, (owners * room, rows), 0) == target[None, :]
        buffer = jnp.dot(
            hot.astype(jnp.bfloat16), tokens, preferred_element_type=jnp.float32
        ).astype(jnp.bfloat16)
        arrived.append(lax.all_to_all(buffer, "expert", split_axis=0, concat_axis=0, tiled=True))

    picked = jnp.zeros((rows, width), jnp.float32)
    for expert in range(held):
        whole_in, whole_out = gathered[expert]
        hidden = jax.nn.relu(
            jnp.dot(arrived[expert], whole_in, preferred_element_type=jnp.float32)
        ).astype(jnp.bfloat16)
        result = jnp.dot(hidden, whole_out, preferred_element_type=jnp.float32).astype(
            jnp.bfloat16
        )
        returned = lax.all_to_all(result, "expert", split_axis=0, concat_axis=0, tiled=True)
        source = jnp.where(which == expert, place, -1)
        hot = source[:, None] == lax.broadcasted_iota(jnp.int32, (rows, owners * room), 1)
        picked = picked + jnp.dot(
            hot.astype(jnp.bfloat16), returned, preferred_element_type=jnp.float32
        )
    return (gate[:, None] * picked).astype(jnp.bfloat16)


def solution(mesh):
    placed = (
        P(("expert", "helper"), None),
        P(("expert", "helper")),
        P(("expert", "helper"), None),
        P(("expert", "helper"), None),
        P(),
        P("expert", None, "helper"),
        P("expert", "helper", None),
    )
    return jax.shard_map(
        on_device,
        mesh=mesh,
        in_specs=placed,
        out_specs=P(("expert", "helper"), None),
        check_vma=False,
    )
```
